32 devices in a mesh: pipe: 2 (over x), tensor: 4 (over y, core), expert: 4 (over z).
Axes of the slice: x: 2, y: 2, z: 4, core: 2. Of those that a mesh axis runs over, the one named last changes fastest.
Arguments:
- tokens: bfloat16 [2, 256, 4096], P(None, 'expert'), may hold values from -6 to 6
- gains: float32 [2, 4096], P('pipe'), may hold values from 0.1 to 1.9
- route_ids: int32 [2, 2, 256, 2], P('pipe', None, 'expert'), may hold values from 0 to 3, all different within a row
- route_weights: float32 [2, 2, 256, 2], P('pipe', None, 'expert'), may hold values from 0.2 to 1
- picks: int32 [2, 2, 4, 64], P('pipe', None, 'expert'), may hold values from 0 to 63, each once within a row
- w_gate: bfloat16 [2, 4, 4096, 1536], P('pipe', 'expert', None, 'tensor'), may hold values from -0.09375 to 0.09375
- w_up: bfloat16 [2, 4, 4096, 1536], P('pipe', 'expert', None, 'tensor'), may hold values from -0.09375 to 0.09375
- w_down: bfloat16 [2, 4, 1536, 4096], P('pipe', 'expert', 'tensor'), may hold values from -0.15625 to 0.15625
Outputs:
- streams: bfloat16 [2, 2, 256, 4096], P('pipe', None, 'expert', 'tensor')
The draws below stay inside these ranges and needn't reach their ends.
Inputs may be any that keep to these rules, and one draw needn't show every extreme that they name: `route_ids`: each token names 2 different experts; every expert is named by some token. `picks`: for every layer, micro-batch and block of 64 tokens, a permutation of 0 to 63.
All inputs are finite; a program needn't handle non-finite values.
Results may differ from the reference program's by a relative error of at most 0.025.
Values may be sent and summed in bfloat16 or wider, within the bound.
A program may use at most 64 MiB of HBM per device.

```python
import jax
import jax.numpy as jnp
from jax import lax

D = 4096
FF = 1536
TOPK = 2
MICRO = 2
TOK_DEV = 64
EXPERTS = 4
QUARTER = 16
CAP = 10
TOKENS = 256
N_PIPE = 2
N_TENSOR = 4
N_EXPERT = 4


def steps_of(rng, shape, shards, low, top_value):
    loudness, own = 1.0, jax.random.fold_in(rng, 6)
    for dim, parts in shards:
        steps = jnp.exp(jax.random.uniform(jax.random.fold_in(own, dim), (parts,), jnp.float32, low / len(shards), top_value / len(shards)))
        loudness = loudness * jnp.repeat(steps, shape[dim] // parts).reshape([-1 if axis == dim else 1 for axis in range(len(shape))])
    return loudness


def different_ones(stream_key, rows, number_of, top, lift):
    sequence = jax.random.permutation(jax.random.fold_in(stream_key, 1), number_of)
    pull = sequence
    for power in range(3):
        pull = pull * pull // number_of
    pull = pull * lift // number_of
    lots = jax.random.randint(jax.random.fold_in(stream_key, 2), (rows, number_of), 0, 4096) + pull
    fixed_rows = jax.random.permutation(jax.random.fold_in(stream_key, 3), rows)[jnp.arange(number_of) % rows]
    lots = jnp.where(jnp.arange(rows)[:, None] == fixed_rows[None, :], 1 << 14, lots)
    priority = lots * number_of + jnp.arange(number_of)
    return lax.top_k(priority.astype(jnp.int32), top)[1].astype(jnp.int32)


def gaussian(key, shape, deviation, most, pieces=(), kind=jnp.bfloat16):
    values = jax.random.normal(key, shape, jnp.float32) * deviation
    if len(pieces) > 0:
        values = steps_of(key, shape, pieces, -0.22, 0.18) * values
    return jnp.clip(values, min=-most, max=most).astype(kind)


def setup_inputs(seed: int = 0) -> dict:
    key_list = jax.random.split(jax.random.key(seed), 9)
    tokens = gaussian(key_list[0], (MICRO, TOKENS, D), 1.0, 6.0, ((1, 4),))
    gains = jnp.clip(1.0 + 0.18 * jax.random.normal(key_list[1], (N_PIPE, D), jnp.float32), 0.1, 1.9)
    route_ids = different_ones(key_list[2], N_PIPE * MICRO * TOKENS, EXPERTS, TOPK, 8192).reshape((N_PIPE, MICRO, TOKENS, TOPK))
    route_weights = jnp.clip(0.2 + 0.8 * jax.random.uniform(key_list[3], (N_PIPE, MICRO, TOKENS, TOPK), jnp.float32) ** steps_of(key_list[3], (N_PIPE, MICRO, TOKENS, TOPK), ((0, 2), (2, 4)), -0.2, 0.2), 0.2, 1.0)
    picks = jax.vmap(lambda own: jax.random.permutation(own, TOK_DEV))(jax.random.split(key_list[4], N_PIPE * MICRO * N_EXPERT)).reshape((N_PIPE, MICRO, N_EXPERT, TOK_DEV)).astype(jnp.int32)
    w_gate = gaussian(key_list[5], (N_PIPE, EXPERTS, D, FF), D ** -0.5, 0.09375, ((0, 2), (1, 4), (3, 4)))
    w_up = gaussian(key_list[6], (N_PIPE, EXPERTS, D, FF), D ** -0.5, 0.09375, ((0, 2), (1, 4), (3, 4)))
    w_down = gaussian(key_list[7], (N_PIPE, EXPERTS, FF, D), FF ** -0.5, 0.15625, ((0, 2), (1, 4), (2, 4)))
    return dict(tokens=tokens, gains=gains, route_ids=route_ids, route_weights=route_weights, picks=picks, w_gate=w_gate, w_up=w_up, w_down=w_down)


epsilon = 1e-06

def find_slots(ordered_ids, capacity):
    onehot = (ordered_ids[..., None] == jnp.arange(EXPERTS, dtype=jnp.int32)).astype(jnp.int32)
    earlier = jnp.cumsum(onehot, axis=-2) - onehot
    slot_index = lax.optimization_barrier(jnp.sum(earlier * onehot, axis=-1))
    return (slot_index, slot_index < capacity)

def expert_ffn(operands):
    row_block, gate_matrix, up_matrix, down_matrix = operands
    gate_val = jnp.dot(row_block, gate_matrix, preferred_element_type=jnp.float32)
    up_val = jnp.dot(row_block, up_matrix, preferred_element_type=jnp.float32)
    hidden = (jax.nn.silu(gate_val) * up_val).astype(jnp.bfloat16)
    shard_width = FF // N_TENSOR
    summed = jnp.zeros((row_block.shape[0], D), jnp.float32)
    for shard_index in range(N_TENSOR):
        lower = shard_index * shard_width
        partial_sum = jnp.dot(hidden[:, lower:lower + shard_width], down_matrix[lower:lower + shard_width], preferred_element_type=jnp.float32)
        rounded = lax.optimization_barrier(partial_sum.astype(jnp.bfloat16))
        summed = summed + rounded.astype(jnp.float32)
    return summed.astype(jnp.bfloat16)

def moe_section(stream, gain_row, section_ids, section_weights, section_picks, gate_all, up_all, down_all):
    groups = N_EXPERT
    offsets = (jnp.arange(groups, dtype=jnp.int32) * TOK_DEV)[:, None]
    ordered = (section_picks + offsets).astype(jnp.int32).reshape(groups, N_TENSOR, QUARTER)
    stream_f = stream.astype(jnp.float32)
    inv_rms = lax.rsqrt(lax.optimization_barrier(jnp.mean(stream_f * stream_f, axis=1, keepdims=True)) + epsilon)
    normed = (stream_f * inv_rms * gain_row[None, :]).astype(jnp.bfloat16)
    ordered_ids = section_ids[ordered].reshape(groups, N_TENSOR, QUARTER * TOPK)
    ordered_weights = section_weights[ordered].reshape(groups, N_TENSOR, QUARTER * TOPK)
    slot_index, kept_mask = find_slots(ordered_ids, CAP)
    route_tokens = jnp.repeat(ordered, TOPK, axis=2)
    group_index = jnp.arange(groups, dtype=jnp.int32)[:, None, None]
    rank_index = jnp.arange(N_TENSOR, dtype=jnp.int32)[None, :, None]
    position = ((ordered_ids * groups + group_index) * N_TENSOR + rank_index) * CAP + slot_index
    filled = EXPERTS * groups * N_TENSOR * CAP
    target = jnp.where(kept_mask, position, filled).astype(jnp.int32)
    source = jnp.full((filled + 1,), TOKENS, jnp.int32).at[target.reshape(-1)].set(route_tokens.reshape(-1))
    padded = jnp.concatenate([normed, jnp.zeros((1, D), jnp.bfloat16)], axis=0)
    row_block = padded[source[:filled]].reshape(EXPERTS, groups * N_TENSOR * CAP, D)
    results = lax.map(expert_ffn, (row_block, gate_all, up_all, down_all))
    flat_results = jnp.concatenate([results.reshape(filled, D), jnp.zeros((1, D), jnp.bfloat16)], axis=0)
    picked = flat_results[target].astype(jnp.float32)
    weighted = picked * (ordered_weights * kept_mask)[..., None]
    update = lax.optimization_barrier(jnp.sum(weighted.reshape(groups, N_TENSOR, QUARTER, TOPK, D), axis=3))
    stream_new = stream_f.at[ordered.reshape(-1)].add(update.reshape(-1, D))
    return stream_new.astype(jnp.bfloat16)

def reference(tokens, gains, route_ids, route_weights, picks, w_gate, w_up, w_down):
    finished = []
    for micro_index in range(MICRO):
        stream = tokens[micro_index]
        column = []
        for section_index in range(N_PIPE):
            stream = moe_section(stream, gains[section_index], route_ids[section_index, micro_index], route_weights[section_index, micro_index], picks[section_index, micro_index], w_gate[section_index], w_up[section_index], w_down[section_index])
            column.append(stream)
        finished.append(jnp.stack(column))
    return jnp.stack(finished, axis=1)
```

```python
import functools

import jax
import jax.numpy as jnp
from jax import lax
from jax.experimental import pallas as pl
from jax.experimental.pallas import tpu as pltpu
from jax.sharding import PartitionSpec as P

epsilon = 1e-06
MESH = pl.DeviceIdType.MESH
F32 = jnp.float32
BF16 = jnp.bfloat16


def layer_kernel(
    sizes, tokens, gains_in, ids_in, weights_in, picks_in, w_gate, w_up, w_down, out,
    gains, ids, weights, picks, placing, comb, h_in, fresh, send, x, wg, wu, wd, g_acc, u_acc, own, p_send, p_recv,
    y_send, y_recv, z_send, ret,
    s_sem, w_sem, o_sem, h_loc, out_sem, h_recv, d_recv, f_recv, c_recv, p_sem, y_sem, z_sem,
):
    micros, n_p, n_t, n_e, pair, parts, rows_ge, width, capacity = sizes
    n_a = n_t // pair
    sub = width // parts
    far_first = list(range(n_e - 1, -1, -1))
    halves = [far_first[0::2], far_first[1::2]]
    halves = [half for half in halves if half]
    ks = range(parts)
    ranks = [(da, dc) for da in range(n_a) for dc in range(pair)]
    p = lax.axis_index("pipe")
    r = lax.axis_index("tensor")
    z = lax.axis_index("expert")
    a = lax.div(r, pair)
    c = lax.rem(r, pair)

    def peer_e(d):
        other = z
        for bit in range(n_e.bit_length()):
            one = 1 << bit
            if d & one:
                other = other + one * (1 - 2 * lax.rem(lax.div(z, one), 2))
        return other

    def rank_of(da, dc):
        return lax.rem(a + da, n_a) * pair + lax.rem(c + dc, pair)

    def remote(src, dst, ssem, rsem, where):
        return pltpu.make_async_remote_copy(
            src_ref=src, dst_ref=dst, send_sem=ssem, recv_sem=rsem,
            device_id=where, device_id_type=MESH,
        )

    loads = [
        pltpu.make_async_copy(w_gate.at[0, 0], wg, w_sem.at[0]),
        pltpu.make_async_copy(w_up.at[0, 0], wu, w_sem.at[1]),
        pltpu.make_async_copy(w_down.at[0, 0], wd, w_sem.at[2]),
    ]

    def first_load(m, k):
        cols = pl.ds(pl.multiple_of(r * width + k * sub, sub), sub)
        return pltpu.make_async_copy(tokens.at[m, :, cols], h_in.at[m, k], h_loc.at[m, k])

    def result(m, k):
        return pltpu.make_async_copy(
            fresh.at[m, k], out.at[0, m, :, k * sub:(k + 1) * sub], o_sem.at[m, k]
        )

    small = [
        pltpu.make_async_copy(src, dst, s_sem.at[i])
        for i, (src, dst) in enumerate(
            [(picks_in, picks), (ids_in, ids), (weights_in, weights), (gains_in, gains)]
        )
    ]
    for load in small:
        load.start()

    @pl.when(p == 0)
    def _():
        for m in range(micros):
            for k in ks:
                first_load(m, k).start()

    for load in loads:
        load.start()

    barrier = pltpu.get_barrier_semaphore()

    def greet(where):
        pl.semaphore_signal(barrier, inc=1, device_id=where, device_id_type=MESH)

    for d in range(1, n_e):
        greet({"expert": peer_e(d)})
    for da in range(1, n_a):
        greet({"tensor": rank_of(da, 0)})
    for dc in range(1, pair):
        greet({"tensor": rank_of(0, dc)})

    @pl.when(p > 0)
    def _():
        greet({"pipe": p - 1})

    @pl.when(p < n_p - 1)
    def _():
        greet({"pipe": p + 1})

    toks = h_in.shape[2]
    quarter = toks // n_t
    down = lax.broadcasted_iota(jnp.int32, (toks, toks), 0)
    across = lax.broadcasted_iota(jnp.int32, (toks, toks), 1)
    same = down == across

    def column(row):
        return jnp.sum(jnp.where(same, row, jnp.zeros_like(row)), axis=1, keepdims=True)

    def row_of(col):
        return jnp.sum(jnp.where(same, col, jnp.zeros_like(col)), axis=0, keepdims=True)

    def slots(m):
        pos = jnp.sum(jnp.where(picks[m] == down, across, 0), axis=1, keepdims=True)
        pos_row = row_of(pos)
        block = lax.div(pos, quarter)
        before = (lax.div(pos_row, quarter) == block) & (pos_row < pos)
        found = []
        for e in range(n_e):
            named = jnp.zeros((1, toks), jnp.int32)
            for k in range(ids.shape[1]):
                named = named + jnp.where(ids[m, k:k + 1] == e, 1, 0)
            slot = jnp.sum(jnp.where(before, named, 0), axis=1, keepdims=True)
            kept = (column(named) > 0) & (slot < capacity)
            found.append(jnp.where(kept, block * capacity + slot, -1))
        return found

    def place(m):
        places = lax.broadcasted_iota(jnp.int32, (rows_ge, toks), 0)
        for e, target in enumerate(slots(m)):
            placing[m, e] = jnp.where(places == row_of(target), 1.0, 0.0).astype(BF16)

    def weigh(m):
        for e, target in enumerate(slots(m)):
            w_row = jnp.zeros((1, toks), F32)
            for k in range(ids.shape[1]):
                w_row = w_row + jnp.where(ids[m, k:k + 1] == e, weights[m, k:k + 1], 0.0)
            spread = lax.broadcasted_iota(jnp.int32, (toks, rows_ge), 1) == target
            w_col = jnp.where(spread, column(w_row), 0.0)
            high = w_col.astype(BF16)
            comb[m, e, :toks] = high
            comb[m, e, toks:] = (w_col - high.astype(F32)).astype(BF16)

    for load in small:
        load.wait()
    place(0)

    ends = jnp.where(p > 0, 1, 0) + jnp.where(p < n_p - 1, 1, 0)
    pl.semaphore_wait(barrier, n_e - 1 + n_a - 1 + pair - 1 + ends)

    def relay(m, k):
        return remote(fresh.at[m, k], h_in.at[m, k], out_sem.at[0], h_recv.at[m, k],
                      {"pipe": jnp.minimum(p + 1, n_p - 1)})

    def d_copy(m, d, k):
        return remote(send.at[m, d, k], x.at[m, r, z, k], out_sem.at[1], d_recv.at[m, d - 1, k],
                      {"expert": peer_e(d)})

    def f_copy(m, d, da, k):
        block = x.at[m, r, peer_e(d), k]
        return remote(block, block, out_sem.at[2], f_recv.at[m, d, da - 1, k],
                      {"tensor": rank_of(da, 0)})

    def c_copy(m, d, da, k):
        block = x.at[m, rank_of(da, 0), peer_e(d), k]
        return remote(block, block, out_sem.at[3], c_recv.at[m, half_of(d), da],
                      {"tensor": rank_of(0, 1)})

    def half_of(d):
        return [h for h, half in enumerate(halves) if d in half][0]

    def shared(m, h, da):
        block = x.at[m, 0, 0:len(halves[h])]
        return remote(block, block, out_sem.at[3], c_recv.at[m, h, da], {"tensor": rank_of(0, 1)})

    def p_copy(m, h, da):
        return remote(p_send.at[m, h, da], p_recv.at[m, h, da], out_sem.at[4],
                      p_sem.at[m, h, da], {"tensor": rank_of(0, 1)})

    def y_copy(m, d, da, k):
        return remote(y_send.at[m, da, d, k], y_recv.at[m, da, d, k], out_sem.at[5],
                      y_sem.at[m, d, da - 1, k], {"tensor": rank_of(da, 0)})

    def z_copy(m, d, k):
        return remote(z_send.at[m, k, d], ret.at[m, k, z], out_sem.at[6], z_sem.at[m, k],
                      {"expert": peer_e(d)})

    def returned(m, k):
        block = ret.at[m, k, 1:n_e]
        return remote(block, block, out_sem.at[6], z_sem.at[m, k], {"expert": peer_e(1)})

    def arrive(m, k, first):
        if first:
            first_load(m, k).wait()
        else:
            relay(m, k).wait_recv()

    def dispatch(m, blocks):
        for d, k in blocks:
            block = jnp.dot(placing[m, peer_e(d)], h_in[m, k], preferred_element_type=F32).astype(BF16)
            if d:
                send[m, d, k] = block
            else:
                x[m, r, z, k] = block
        for d, k in blocks:
            if d:
                d_copy(m, d, k).start()

    def forward(m, d):
        for k in ks:
            if d:
                d_copy(m, d, k).wait_recv()
            for da in range(1, n_a):
                f_copy(m, d, da, k).start()
            if pair > 1:
                c_copy(m, d, 0, k).start()

    def pass_on(m, d):
        for k in ks:
            for da in range(1, n_a):
                f_copy(m, d, da, k).wait_recv()
                if pair > 1:
                    c_copy(m, d, da, k).start()

    squares = {}

    def gate(m, h, i):
        da, dc = ranks[i]
        if m == 0 and h == 0 and i == 0:
            loads[0].wait()
            loads[1].wait()
        if dc:
            shared(m, h, da).wait_recv()
        q = rank_of(da, dc)
        gq = uq = None
        ss = squares.get((m, h))
        for k in ks:
            xf = jnp.concatenate([x[m, q, peer_e(d), k].astype(F32) for d in halves[h]], axis=0)
            part = jnp.sum(xf * xf, axis=-1, keepdims=True)
            ss = part if ss is None else ss + part
            start = pl.multiple_of(q * width + k * sub, sub)
            xg = (xf * gains[0:1, pl.ds(start, sub)]).astype(BF16)
            g1 = jnp.dot(xg, wg[pl.ds(start, sub), :], preferred_element_type=F32)
            u1 = jnp.dot(xg, wu[pl.ds(start, sub), :], preferred_element_type=F32)
            gq = g1 if gq is None else gq + g1
            uq = u1 if uq is None else uq + u1
        squares[m, h] = ss
        if i == 0:
            g_acc[...] = gq
            u_acc[...] = uq
        else:
            g_acc[...] += gq
            u_acc[...] += uq

    def finish(m, h):
        if m == 0 and h == 0:
            loads[2].wait()
        inv = lax.rsqrt(squares[m, h] * (1.0 / (n_t * width)) + epsilon)
        g = g_acc[...] * inv
        hidden = (g / (1.0 + jnp.exp(-g)) * (u_acc[...] * inv)).astype(BF16)
        order = list(range(1, n_a)) + [0]
        for dc in list(range(1, pair)) + [0]:
            for da in order:
                for k in ks:
                    start = pl.multiple_of(rank_of(da, dc) * width + k * sub, sub)
                    part = jnp.dot(hidden, wd[:, pl.ds(start, sub)], preferred_element_type=F32)
                    if dc:
                        p_send[m, h, da, k] = part.astype(BF16)
                    else:
                        own[m, h, da, k] = part.astype(BF16)
            if dc:
                for da in order:
                    p_copy(m, h, da).start()

    def reduce_pair(m, h):
        for da in list(range(1, n_a)) + [0]:
            if pair > 1:
                p_copy(m, h, da).wait_recv()
            for i, d in enumerate(halves[h]):
                for k in ks:
                    part = slice(i * rows_ge, (i + 1) * rows_ge)
                    total = own[m, h, da, k, part].astype(F32)
                    if pair > 1:
                        total = total + p_recv[m, h, da, k, part].astype(F32)
                    y_send[m, da, d, k] = total.astype(BF16)
                    if da:
                        y_copy(m, d, da, k).start()

    def reduce_far(m, d):
        for k in ks:
            total = y_send[m, 0, d, k].astype(F32)
            for da in range(1, n_a):
                y_copy(m, d, da, k).wait_recv()
                total = total + y_recv[m, da, d, k].astype(F32)
            if d:
                z_send[m, k, d] = total.astype(BF16)
                z_copy(m, d, k).start()
            else:
                ret[m, k, z] = total.astype(BF16)

    def combine(m):
        for k in ks:
            returned(m, k).wait_recv()
            for d in range(n_e):
                e = peer_e(d)
                both = jnp.dot(comb[m, e], ret[m, k, e], preferred_element_type=F32)
                g_part = both[:toks] + both[toks:]
                update = g_part if d == 0 else update + g_part
            fresh[m, k] = (h_in[m, k].astype(F32) + update).astype(BF16)

            @pl.when(p < n_p - 1)
            def _():
                relay(m, k).start()

            result(m, k).start()

    def step(fn, *args):
        return functools.partial(fn, *args)

    near, rest = halves[0], [d for d in halves[1] if d]
    last = len(ranks)

    def spread(m, first):
        order = near + rest + [0]
        if first:
            steps = [step(arrive, m, k, first) for k in ks]
            return steps + [step(dispatch, m, [(d, k) for d in order for k in ks])]
        steps = []
        for k in ks:
            steps += [step(arrive, m, k, first), step(dispatch, m, [(d, k) for d in order])]
        return steps

    def gates(m, h, low, high):
        return [step(gate, m, h, i) for i in range(low, high)]

    def each(fn, m, blocks):
        return [step(fn, m, d) for d in blocks]

    def plan_for(first):
        plan = []
        if not first:
            plan += [step(place, m) for m in range(1, micros)]
            plan += [step(weigh, m) for m in range(micros)]
        plan += spread(0, first) + [step(forward, 0, 0)]
        if first:
            plan += [step(place, m) for m in range(1, micros)]
        for m in range(micros):
            ahead = first and m
            more = m + 1 < micros
            plan += each(pass_on, m, [0])
            if not ahead:
                plan += each(forward, m, near)
            plan += gates(m, 0, 0, pair)
            if ahead:
                plan += [step(combine, m - 1)]
            plan += each(pass_on, m, near)
            plan += gates(m, 0, pair, last - 1)
            if not ahead:
                plan += each(forward, m, rest)
            if first and m == 0:
                for n in range(1, micros):
                    plan += spread(n, first)
            plan += gates(m, 0, last - 1, last)
            plan += [step(finish, m, 0)]
            plan += gates(m, 1, 0, pair)
            plan += [step(reduce_pair, m, 0)]
            if m and not first:
                plan += [step(combine, m - 1)]
            plan += each(pass_on, m, rest)
            plan += gates(m, 1, pair, last - 1)
            if first:
                plan += [step(weigh, m)]
            plan += gates(m, 1, last - 1, last)
            plan += [step(finish, m, 1)]
            plan += each(reduce_far, m, near[:1])
            plan += [step(reduce_pair, m, 1)]
            if more:
                if first:
                    plan += each(forward, m + 1, [0] + near + rest)
                else:
                    plan += spread(m + 1, first)
                    plan += each(forward, m + 1, [0])
            plan += each(reduce_far, m, near[1:] + rest + [0])
        plan += [step(combine, micros - 1)]
        return plan

    def follow(first):
        squares.clear()
        for go in plan_for(first):
            go()

    @pl.when(p == 0)
    def _():
        follow(True)

    @pl.when(p > 0)
    def _():
        follow(False)

    def sent(block, i):
        remote(block, block, out_sem.at[i], out_sem.at[i], {"expert": peer_e(1)}).wait_send()

    sent(send.at[:, 1:n_e], 1)
    if n_a > 1:
        sent(x.at[:, 0:n_a - 1], 2)
        sent(y_send.at[:, 1:n_a], 5)
    if pair > 1:
        sent(x.at[:, 0:n_a], 3)
        sent(p_send, 4)
    sent(z_send.at[:, :, 1:n_e], 6)
    for m in range(micros):
        for k in ks:
            result(m, k).wait()

    @pl.when(p < n_p - 1)
    def _():
        sent(fresh, 0)


def local(mesh_shape, tokens, gains, route_ids, route_weights, picks, w_gate, w_up, w_down):
    n_p, n_t, n_e = mesh_shape
    micros, toks, model_width = tokens.shape
    route_count = route_ids.shape[3]
    quarter = toks // n_t
    capacity = 4 * quarter * route_count // (3 * n_e)
    width = model_width // n_t
    pair = 2 if n_t % 2 == 0 else 1
    parts = 2 if width % 256 == 0 else 1
    sub = width // parts
    n_a = n_t // pair
    rows_ge = -(-n_t * capacity // 8) * 8
    rows = (n_e + 1) // 2 * rows_ge
    hidden_width = w_gate.shape[3]

    ids = route_ids[0].transpose(0, 2, 1)
    weights = route_weights[0].transpose(0, 2, 1)
    order = picks[0]

    sizes = (micros, n_p, n_t, n_e, pair, parts, rows_ge, width, capacity)
    dma = pltpu.SemaphoreType.DMA
    pinned = pl.BlockSpec(memory_space=pl.ANY)
    return pl.pallas_call(
        functools.partial(layer_kernel, sizes),
        out_shape=jax.ShapeDtypeStruct((1, micros, toks, width), BF16),
        in_specs=[pinned] * 8,
        out_specs=pinned,
        scratch_shapes=[
            pltpu.VMEM(gains.shape, F32),
            pltpu.VMEM(ids.shape, jnp.int32),
            pltpu.VMEM(weights.shape, F32),
            pltpu.VMEM(order.shape, jnp.int32),
            pltpu.VMEM((micros, n_e, rows_ge, toks), BF16),
            pltpu.VMEM((micros, n_e, 2 * toks, rows_ge), BF16),
            pltpu.VMEM((micros, parts, toks, sub), BF16),
            pltpu.VMEM((micros, parts, toks, sub), BF16),
            pltpu.VMEM((micros, n_e, parts, rows_ge, sub), BF16),
            pltpu.VMEM((micros, n_t, n_e, parts, rows_ge, sub), BF16),
            pltpu.VMEM(w_gate.shape[2:], BF16),
            pltpu.VMEM(w_up.shape[2:], BF16),
            pltpu.VMEM(w_down.shape[2:], BF16),
            pltpu.VMEM((rows, hidden_width), F32),
            pltpu.VMEM((rows, hidden_width), F32),
            pltpu.VMEM((micros, 2, n_a, parts, rows, sub), BF16),
            pltpu.VMEM((micros, 2, n_a, parts, rows, sub), BF16),
            pltpu.VMEM((micros, 2, n_a, parts, rows, sub), BF16),
            pltpu.VMEM((micros, n_a, n_e, parts, rows_ge, sub), BF16),
            pltpu.VMEM((micros, n_a, n_e, parts, rows_ge, sub), BF16),
            pltpu.VMEM((micros, parts, n_e, rows_ge, sub), BF16),
            pltpu.VMEM((micros, parts, n_e, rows_ge, sub), BF16),
            dma((4,)), dma((3,)), dma((micros, parts)), dma((micros, parts)),
            dma((7,)), dma((micros, parts)), dma((micros, n_e - 1, parts)),
            dma((micros, n_e, n_a - 1, parts)), dma((micros, 2, n_a)), dma((micros, 2, n_a)),
            dma((micros, n_e, n_a - 1, parts)), dma((micros, parts)),
        ],
        compiler_params=pltpu.CompilerParams(
            collective_id=0, has_side_effects=True, vmem_limit_bytes=67043328
        ),
    )(tokens, gains, ids, weights, order, w_gate, w_up, w_down)


def solution(mesh):
    mesh_shape = (mesh.shape["pipe"], mesh.shape["tensor"], mesh.shape["expert"])
    return jax.shard_map(
        functools.partial(local, mesh_shape),
        mesh=mesh,
        in_specs=(
            P(None, "expert", None),
            P("pipe", None),
            P("pipe", None, "expert", None),
            P("pipe", None, "expert", None),
            P("pipe", None, "expert", None),
            P("pipe", "expert", None, "tensor"),
            P("pipe", "expert", None, "tensor"),
            P("pipe", "expert", "tensor", None),
        ),
        out_specs=P("pipe", None, "expert", "tensor"),
        check_vma=False,
    )
```

```python
import functools

import jax
import jax.numpy as jnp
from jax import lax
from jax.experimental import pallas as pl
from jax.experimental.pallas import tpu as pltpu
from jax.sharding import PartitionSpec as P

epsilon = 1e-06
MESH = pl.DeviceIdType.MESH
F32 = jnp.float32
BF16 = jnp.bfloat16


def layer_kernel(
    sizes, tokens, gains_in, ids_in, weights_in, picks_in, w_gate, w_up, w_down, out,
    gains, ids, weights, picks, placing, comb, h_in, fresh, send, x, wg, wu, wd, g_acc, u_acc, own, p_send, p_recv,
    y_send, y_recv, z_send, ret,
    s_sem, w_sem, o_sem, h_loc, out_sem, h_recv, d_recv, f_recv, c_recv, p_sem, y_sem, z_sem,
):
    micros, n_p, n_t, n_e, pair, parts, rows_ge, width, capacity = sizes
    n_a = n_t // pair
    sub = width // parts
    far_first = list(range(n_e - 1, -1, -1))
    halves = [far_first[0::2], far_first[1::2]]
    halves = [half for half in halves if half]
    ks = range(parts)
    ranks = [(da, dc) for da in range(n_a) for dc in range(pair)]
    p = lax.axis_index("pipe")
    r = lax.axis_index("tensor")
    z = lax.axis_index("expert")
    a = lax.div(r, pair)
    c = lax.rem(r, pair)

    def peer_e(d):
        other = z
        for bit in range(n_e.bit_length()):
            one = 1 << bit
            if d & one:
                other = other + one * (1 - 2 * lax.rem(lax.div(z, one), 2))
        return other

    def rank_of(da, dc):
        return lax.rem(a + da, n_a) * pair + lax.rem(c + dc, pair)

    def remote(src, dst, ssem, rsem, where):
        return pltpu.make_async_remote_copy(
            src_ref=src, dst_ref=dst, send_sem=ssem, recv_sem=rsem,
            device_id=where, device_id_type=MESH,
        )

    loads = [
        pltpu.make_async_copy(w_gate.at[0, 0], wg, w_sem.at[0]),
        pltpu.make_async_copy(w_up.at[0, 0], wu, w_sem.at[1]),
        pltpu.make_async_copy(w_down.at[0, 0], wd, w_sem.at[2]),
    ]

    def first_load(m, k):
        cols = pl.ds(pl.multiple_of(r * width + k * sub, sub), sub)
        return pltpu.make_async_copy(tokens.at[m, :, cols], h_in.at[m, k], h_loc.at[m, k])

    def result(m, k):
        return pltpu.make_async_copy(
            fresh.at[m, k], out.at[0, m, :, k * sub:(k + 1) * sub], o_sem.at[m, k]
        )

    small = [
        pltpu.make_async_copy(src, dst, s_sem.at[i])
        for i, (src, dst) in enumerate(
            [(picks_in, picks), (ids_in, ids), (weights_in, weights), (gains_in, gains)]
        )
    ]
    for load in small:
        load.start()

    @pl.when(p == 0)
    def _():
        for m in range(micros):
            for k in ks:
                first_load(m, k).start()

    barrier = pltpu.get_barrier_semaphore()

    def greet(where):
        pl.semaphore_signal(barrier, inc=1, device_id=where, device_id_type=MESH)

    for d in range(1, n_e):
        greet({"expert": peer_e(d)})
    for da in range(1, n_a):
        greet({"tensor": rank_of(da, 0)})
    for dc in range(1, pair):
        greet({"tensor": rank_of(0, dc)})

    @pl.when(p > 0)
    def _():
        greet({"pipe": p - 1})

    @pl.when(p < n_p - 1)
    def _():
        greet({"pipe": p + 1})

    toks = h_in.shape[2]
    quarter = toks // n_t
    down = lax.broadcasted_iota(jnp.int32, (toks, toks), 0)
    across = lax.broadcasted_iota(jnp.int32, (toks, toks), 1)
    same = down == across

    def column(row):
        return jnp.sum(jnp.where(same, row, jnp.zeros_like(row)), axis=1, keepdims=True)

    def row_of(col):
        return jnp.sum(jnp.where(same, col, jnp.zeros_like(col)), axis=0, keepdims=True)

    def slots(m):
        pos = jnp.sum(jnp.where(picks[m] == down, across, 0), axis=1, keepdims=True)
        pos_row = row_of(pos)
        block = lax.div(pos, quarter)
        before = (lax.div(pos_row, quarter) == block) & (pos_row < pos)
        found = []
        for e in range(n_e):
            named = jnp.zeros((1, toks), jnp.int32)
            for k in range(ids.shape[1]):
                named = named + jnp.where(ids[m, k:k + 1] == e, 1, 0)
            slot = jnp.sum(jnp.where(before, named, 0), axis=1, keepdims=True)
            kept = (column(named) > 0) & (slot < capacity)
            found.append(jnp.where(kept, block * capacity + slot, -1))
        return found

    def place(m):
        places = lax.broadcasted_iota(jnp.int32, (rows_ge, toks), 0)
        for e, target in enumerate(slots(m)):
            placing[m, e] = jnp.where(places == row_of(target), 1.0, 0.0).astype(BF16)

    def weigh(m):
        for e, target in enumerate(slots(m)):
            w_row = jnp.zeros((1, toks), F32)
            for k in range(ids.shape[1]):
                w_row = w_row + jnp.where(ids[m, k:k + 1] == e, weights[m, k:k + 1], 0.0)
            spread = lax.broadcasted_iota(jnp.int32, (toks, rows_ge), 1) == target
            w_col = jnp.where(spread, column(w_row), 0.0)
            high = w_col.astype(BF16)
            comb[m, e, :toks] = high
            comb[m, e, toks:] = (w_col - high.astype(F32)).astype(BF16)

    for load in small:
        load.wait()
    for load in loads:
        load.start()
    place(0)

    ends = jnp.where(p > 0, 1, 0) + jnp.where(p < n_p - 1, 1, 0)
    pl.semaphore_wait(barrier, n_e - 1 + n_a - 1 + pair - 1 + ends)

    def relay(m, k):
        return remote(fresh.at[m, k], h_in.at[m, k], out_sem.at[0], h_recv.at[m, k],
                      {"pipe": jnp.minimum(p + 1, n_p - 1)})

    def d_copy(m, d, k):
        return remote(send.at[m, d, k], x.at[m, r, z, k], out_sem.at[1], d_recv.at[m, d - 1, k],
                      {"expert": peer_e(d)})

    def f_copy(m, d, da, k):
        block = x.at[m, r, peer_e(d), k]
        return remote(block, block, out_sem.at[2], f_recv.at[m, d, da - 1, k],
                      {"tensor": rank_of(da, 0)})

    def c_copy(m, d, da, k):
        block = x.at[m, rank_of(da, 0), peer_e(d), k]
        return remote(block, block, out_sem.at[3], c_recv.at[m, half_of(d), da],
                      {"tensor": rank_of(0, 1)})

    def half_of(d):
        return [h for h, half in enumerate(halves) if d in half][0]

    def shared(m, h, da):
        block = x.at[m, 0, 0:len(halves[h])]
        return remote(block, block, out_sem.at[3], c_recv.at[m, h, da], {"tensor": rank_of(0, 1)})

    def p_copy(m, h, da):
        return remote(p_send.at[m, h, da], p_recv.at[m, h, da], out_sem.at[4],
                      p_sem.at[m, h, da], {"tensor": rank_of(0, 1)})

    def y_copy(m, d, da, k):
        return remote(y_send.at[m, da, d, k], y_recv.at[m, da, d, k], out_sem.at[5],
                      y_sem.at[m, d, da - 1, k], {"tensor": rank_of(da, 0)})

    def z_copy(m, d, k):
        return remote(z_send.at[m, k, d], ret.at[m, k, z], out_sem.at[6], z_sem.at[m, k],
                      {"expert": peer_e(d)})

    def returned(m, k):
        block = ret.at[m, k, 1:n_e]
        return remote(block, block, out_sem.at[6], z_sem.at[m, k], {"expert": peer_e(1)})

    def arrive(m, k, first):
        if first:
            first_load(m, k).wait()
        else:
            relay(m, k).wait_recv()

    def dispatch(m, blocks):
        for d, k in blocks:
            block = jnp.dot(placing[m, peer_e(d)], h_in[m, k], preferred_element_type=F32).astype(BF16)
            if d:
                send[m, d, k] = block
            else:
                x[m, r, z, k] = block
        for d, k in blocks:
            if d:
                d_copy(m, d, k).start()

    def forward(m, d, k):
        if d:
            d_copy(m, d, k).wait_recv()
        for da in range(1, n_a):
            f_copy(m, d, da, k).start()
        if pair > 1:
            c_copy(m, d, 0, k).start()

    def pass_on(m, d, k):
        for da in range(1, n_a):
            f_copy(m, d, da, k).wait_recv()
            if pair > 1:
                c_copy(m, d, da, k).start()

    squares = {}

    def gate(m, h, i):
        da, dc = ranks[i]
        if m == 0 and h == 0 and i == 0:
            loads[0].wait()
            loads[1].wait()
        if dc:
            shared(m, h, da).wait_recv()
        q = rank_of(da, dc)
        gq = uq = None
        ss = squares.get((m, h))
        for k in ks:
            xf = jnp.concatenate([x[m, q, peer_e(d), k].astype(F32) for d in halves[h]], axis=0)
            part = jnp.sum(xf * xf, axis=-1, keepdims=True)
            ss = part if ss is None else ss + part
            start = pl.multiple_of(q * width + k * sub, sub)
            xg = (xf * gains[0:1, pl.ds(start, sub)]).astype(BF16)
            g1 = jnp.dot(xg, wg[pl.ds(start, sub), :], preferred_element_type=F32)
            u1 = jnp.dot(xg, wu[pl.ds(start, sub), :], preferred_element_type=F32)
            gq = g1 if gq is None else gq + g1
            uq = u1 if uq is None else uq + u1
        squares[m, h] = ss
        if i == 0:
            g_acc[h] = gq
            u_acc[h] = uq
        else:
            g_acc[h] += gq
            u_acc[h] += uq

    def finish(m, h):
        if m == 0 and h == 0:
            loads[2].wait()
        inv = lax.rsqrt(squares[m, h] * (1.0 / (n_t * width)) + epsilon)
        g = g_acc[h] * inv
        hidden = (g / (1.0 + jnp.exp(-g)) * (u_acc[h] * inv)).astype(BF16)
        order = list(range(1, n_a)) + [0]
        for dc in list(range(1, pair)) + [0]:
            for da in order:
                for k in ks:
                    start = pl.multiple_of(rank_of(da, dc) * width + k * sub, sub)
                    part = jnp.dot(hidden, wd[:, pl.ds(start, sub)], preferred_element_type=F32)
                    if dc:
                        p_send[m, h, da, k] = part.astype(BF16)
                    else:
                        own[m, h, da, k] = part.astype(BF16)
            if dc:
                for da in order:
                    p_copy(m, h, da).start()

    def reduce_pair(m, h):
        for da in list(range(1, n_a)) + [0]:
            if pair > 1:
                p_copy(m, h, da).wait_recv()
            for i, d in enumerate(halves[h]):
                for k in ks:
                    part = slice(i * rows_ge, (i + 1) * rows_ge)
                    total = own[m, h, da, k, part].astype(F32)
                    if pair > 1:
                        total = total + p_recv[m, h, da, k, part].astype(F32)
                    y_send[m, da, d, k] = total.astype(BF16)
                    if da:
                        y_copy(m, d, da, k).start()

    def reduce_far(m, d, k):
        total = y_send[m, 0, d, k].astype(F32)
        for da in range(1, n_a):
            y_copy(m, d, da, k).wait_recv()
            total = total + y_recv[m, da, d, k].astype(F32)
        if d:
            z_send[m, k, d] = total.astype(BF16)
            z_copy(m, d, k).start()
        else:
            ret[m, k, z] = total.astype(BF16)

    def combine(m, k):
        returned(m, k).wait_recv()
        for d in range(n_e):
            e = peer_e(d)
            both = jnp.dot(comb[m, e], ret[m, k, e], preferred_element_type=F32)
            g_part = both[:toks] + both[toks:]
            update = g_part if d == 0 else update + g_part
        fresh[m, k] = (h_in[m, k].astype(F32) + update).astype(BF16)

        @pl.when(p < n_p - 1)
        def _():
            relay(m, k).start()

        result(m, k).start()

    def step(fn, *args):
        return functools.partial(fn, *args)

    near, rest = halves[0], [d for d in halves[1] if d]
    last = len(ranks)

    def gates(m, h, low, high):
        return [step(gate, m, h, i) for i in range(low, high)]

    def each(fn, m, blocks, parts_of=ks):
        return [step(fn, m, d, k) for d in blocks for k in parts_of]

    def spread(m, first):
        steps = []
        for k in ks:
            steps += [step(arrive, m, k, first), step(dispatch, m, [(d, k) for d in near])]
        for k in ks:
            steps += [step(dispatch, m, [(d, k) for d in rest])]
        return steps

    def keep(m):
        return [step(dispatch, m, [(0, k) for k in ks])] + each(forward, m, [0])

    early, late = list(ks)[:-1], list(ks)[-1:]

    def body(m, ahead, between, held):
        plan = each(forward, m, near) + gates(m, 0, 0, 1)
        plan += each(forward, m, rest, early) + each(pass_on, m, near[:1], early)
        plan += gates(m, 0, 1, pair) + ahead
        plan += each(pass_on, m, [0]) + each(pass_on, m, near[:1], late) + each(pass_on, m, near[1:])
        plan += gates(m, 0, pair, last - 1)
        plan += each(forward, m, rest, late) + held + between
        plan += gates(m, 1, 0, 1)
        plan += gates(m, 0, last - 1, last)
        plan += [step(finish, m, 0)]
        plan += each(pass_on, m, rest, early)
        plan += gates(m, 1, 1, pair)
        plan += [step(reduce_pair, m, 0)]
        plan += each(pass_on, m, rest, late)
        plan += gates(m, 1, pair, last)
        plan += [step(finish, m, 1)]
        return plan

    def joined(m):
        return [step(combine, m, k) for k in ks]

    def first_plan():
        close = near[1:]
        plan = spread(0, True) + keep(0)
        for m in range(1, micros):
            plan += [step(place, m)] + [step(arrive, m, k, True) for k in ks] + keep(m)
        for m in range(micros):
            more = range(m + 1, min(m + 2, micros))
            far = [step(dispatch, n, [(d, k) for d in near[:1] + rest for k in ks]) for n in more]
            side = [step(dispatch, n, [(d, k) for d in close for k in ks]) for n in more]
            if m == 0:
                moved = [go for n in more for go in each(forward, n, close)]
                plan += side + body(m, far, moved, [])
            else:
                plan += gates(m, 0, 0, 1) + joined(m - 1)
                plan += side + far + [go for n in more for go in each(forward, n, close)]
                plan += each(pass_on, m, [0] + close) + gates(m, 0, 1, pair) + each(pass_on, m, near[:1])
                plan += gates(m, 0, pair, last) + [step(finish, m, 0)]
                plan += each(pass_on, m, rest, early) + gates(m, 1, 0, pair) + [step(reduce_pair, m, 0)]
                plan += each(pass_on, m, rest, late) + gates(m, 1, pair, last) + [step(finish, m, 1)]
            plan += [step(weigh, m)]
            plan += each(reduce_far, m, near[:1], early) + [step(reduce_pair, m, 1)]
            plan += each(reduce_far, m, near[:1], late)
            for n in more:
                plan += each(forward, n, near[:1])
            plan += each(reduce_far, m, close)
            for n in more:
                plan += each(forward, n, rest)
            plan += each(reduce_far, m, rest + [0])
        return plan + joined(micros - 1)

    def later_plan():
        plan = [step(place, m) for m in range(1, micros)] + [step(weigh, m) for m in range(micros)]
        for m in range(micros):
            held = each(reduce_far, m - 1, near + rest + [0]) if m else []
            plan += spread(m, False) + keep(m) + body(m, [], [], held)
            if m + 1 == micros:
                plan += each(reduce_far, m, near[:1], early)
            plan += [step(reduce_pair, m, 1)]
            if m:
                plan += joined(m - 1)
        plan += each(reduce_far, micros - 1, near[:1], late)
        plan += each(reduce_far, micros - 1, near[1:] + rest + [0])
        return plan + joined(micros - 1)

    def follow(first):
        squares.clear()
        for go in first_plan() if first else later_plan():
            go()

    @pl.when(p == 0)
    def _():
        follow(True)

    @pl.when(p > 0)
    def _():
        follow(False)

    def sent(block, i):
        remote(block, block, out_sem.at[i], out_sem.at[i], {"expert": peer_e(1)}).wait_send()

    sent(send.at[:, 1:n_e], 1)
    if n_a > 1:
        sent(x.at[:, 0:n_a - 1], 2)
        sent(y_send.at[:, 1:n_a], 5)
    if pair > 1:
        sent(x.at[:, 0:n_a], 3)
        sent(p_send, 4)
    sent(z_send.at[:, :, 1:n_e], 6)
    for m in range(micros):
        for k in ks:
            result(m, k).wait()

    @pl.when(p < n_p - 1)
    def _():
        sent(fresh, 0)


def local(mesh_shape, tokens, gains, route_ids, route_weights, picks, w_gate, w_up, w_down):
    n_p, n_t, n_e = mesh_shape
    micros, toks, model_width = tokens.shape
    route_count = route_ids.shape[3]
    quarter = toks // n_t
    capacity = 4 * quarter * route_count // (3 * n_e)
    width = model_width // n_t
    pair = 2 if n_t % 2 == 0 else 1
    parts = 2 if width % 256 == 0 else 1
    sub = width // parts
    n_a = n_t // pair
    rows_ge = -(-n_t * capacity // 8) * 8
    rows = (n_e + 1) // 2 * rows_ge
    hidden_width = w_gate.shape[3]

    ids = route_ids[0].transpose(0, 2, 1)
    weights = route_weights[0].transpose(0, 2, 1)
    order = picks[0]

    sizes = (micros, n_p, n_t, n_e, pair, parts, rows_ge, width, capacity)
    dma = pltpu.SemaphoreType.DMA
    pinned = pl.BlockSpec(memory_space=pl.ANY)
    return pl.pallas_call(
        functools.partial(layer_kernel, sizes),
        out_shape=jax.ShapeDtypeStruct((1, micros, toks, width), BF16),
        in_specs=[pinned] * 8,
        out_specs=pinned,
        scratch_shapes=[
            pltpu.VMEM(gains.shape, F32),
            pltpu.VMEM(ids.shape, jnp.int32),
            pltpu.VMEM(weights.shape, F32),
            pltpu.VMEM(order.shape, jnp.int32),
            pltpu.VMEM((micros, n_e, rows_ge, toks), BF16),
            pltpu.VMEM((micros, n_e, 2 * toks, rows_ge), BF16),
            pltpu.VMEM((micros, parts, toks, sub), BF16),
            pltpu.VMEM((micros, parts, toks, sub), BF16),
            pltpu.VMEM((micros, n_e, parts, rows_ge, sub), BF16),
            pltpu.VMEM((micros, n_t, n_e, parts, rows_ge, sub), BF16),
            pltpu.VMEM(w_gate.shape[2:], BF16),
            pltpu.VMEM(w_up.shape[2:], BF16),
            pltpu.VMEM(w_down.shape[2:], BF16),
            pltpu.VMEM((2, rows, hidden_width), F32),
            pltpu.VMEM((2, rows, hidden_width), F32),
            pltpu.VMEM((micros, 2, n_a, parts, rows, sub), BF16),
            pltpu.VMEM((micros, 2, n_a, parts, rows, sub), BF16),
            pltpu.VMEM((micros, 2, n_a, parts, rows, sub), BF16),
            pltpu.VMEM((micros, n_a, n_e, parts, rows_ge, sub), BF16),
            pltpu.VMEM((micros, n_a, n_e, parts, rows_ge, sub), BF16),
            pltpu.VMEM((micros, parts, n_e, rows_ge, sub), BF16),
            pltpu.VMEM((micros, parts, n_e, rows_ge, sub), BF16),
            dma((4,)), dma((3,)), dma((micros, parts)), dma((micros, parts)),
            dma((7,)), dma((micros, parts)), dma((micros, n_e - 1, parts)),
            dma((micros, n_e, n_a - 1, parts)), dma((micros, 2, n_a)), dma((micros, 2, n_a)),
            dma((micros, n_e, n_a - 1, parts)), dma((micros, parts)),
        ],
        compiler_params=pltpu.CompilerParams(
            collective_id=0, has_side_effects=True, vmem_limit_bytes=67043328
        ),
    )(tokens, gains, ids, weights, order, w_gate, w_up, w_down)


def solution(mesh):
    mesh_shape = (mesh.shape["pipe"], mesh.shape["tensor"], mesh.shape["expert"])
    return jax.shard_map(
        functools.partial(local, mesh_shape),
        mesh=mesh,
        in_specs=(
            P(None, "expert", None),
            P("pipe", None),
            P("pipe", None, "expert", None),
            P("pipe", None, "expert", None),
            P("pipe", None, "expert", None),
            P("pipe", "expert", None, "tensor"),
            P("pipe", "expert", None, "tensor"),
            P("pipe", "expert", "tensor", None),
        ),
        out_specs=P("pipe", None, "expert", "tensor"),
        check_vma=False,
    )
```

```python
import functools

import jax
import jax.numpy as jnp
from jax import lax
from jax.experimental import pallas as pl
from jax.experimental.pallas import tpu as pltpu
from jax.sharding import PartitionSpec as P

epsilon = 1e-06
MESH = pl.DeviceIdType.MESH
F32 = jnp.float32
BF16 = jnp.bfloat16


def layer_kernel(
    sizes, tokens, gains_in, ids_in, weights_in, picks_in, w_gate, w_up, w_down, out,
    gains, ids, weights, picks, placing, comb, h_in, fresh, send, x, wg, wu, wd, g_acc, u_acc, own, p_send, p_recv,
    y_send, y_recv, z_send, ret,
    s_sem, w_sem, h_loc, out_sem, h_recv, d_recv, f_recv, c_recv, p_sem, y_sem, z_sem,
):
    micros, n_p, n_t, n_e, pair, parts, rows_ge, width, capacity = sizes
    n_a = n_t // pair
    sub = width // parts
    far_first = list(range(n_e - 1, -1, -1))
    halves = [far_first[0::2], far_first[1::2]]
    halves = [half for half in halves if half]
    ks = range(parts)
    ranks = [(da, dc) for da in range(n_a) for dc in range(pair)]
    p = lax.axis_index("pipe")
    r = lax.axis_index("tensor")
    z = lax.axis_index("expert")
    a = lax.div(r, pair)
    c = lax.rem(r, pair)

    def peer_e(d):
        other = z
        for bit in range(n_e.bit_length()):
            one = 1 << bit
            if d & one:
                other = other + one * (1 - 2 * lax.rem(lax.div(z, one), 2))
        return other

    def rank_of(da, dc):
        return lax.rem(a + da, n_a) * pair + lax.rem(c + dc, pair)

    def remote(src, dst, ssem, rsem, where):
        return pltpu.make_async_remote_copy(
            src_ref=src, dst_ref=dst, send_sem=ssem, recv_sem=rsem,
            device_id=where, device_id_type=MESH,
        )

    loads = [
        pltpu.make_async_copy(w_gate.at[0, 0], wg, w_sem.at[0]),
        pltpu.make_async_copy(w_up.at[0, 0], wu, w_sem.at[1]),
        pltpu.make_async_copy(w_down.at[0, 0], wd, w_sem.at[2]),
    ]

    def first_load(m, k):
        cols = pl.ds(pl.multiple_of(r * width + k * sub, sub), sub)
        return pltpu.make_async_copy(tokens.at[m, :, cols], h_in.at[m, k], h_loc.at[m, k])

    small = [
        pltpu.make_async_copy(src, dst, s_sem.at[i])
        for i, (src, dst) in enumerate(
            [(picks_in, picks), (ids_in, ids), (weights_in, weights), (gains_in, gains)]
        )
    ]
    for load in small:
        load.start()

    @pl.when(p == 0)
    def _():
        for m in range(micros):
            for k in ks:
                first_load(m, k).start()

    barrier = pltpu.get_barrier_semaphore()

    def greet(where):
        pl.semaphore_signal(barrier, inc=1, device_id=where, device_id_type=MESH)

    for d in range(1, n_e):
        greet({"expert": peer_e(d)})
    for da in range(1, n_a):
        greet({"tensor": rank_of(da, 0)})
    for dc in range(1, pair):
        greet({"tensor": rank_of(0, dc)})

    @pl.when(p > 0)
    def _():
        greet({"pipe": p - 1})

    @pl.when(p < n_p - 1)
    def _():
        greet({"pipe": p + 1})

    toks = h_in.shape[2]
    quarter = toks // n_t
    down = lax.broadcasted_iota(jnp.int32, (toks, toks), 0)
    across = lax.broadcasted_iota(jnp.int32, (toks, toks), 1)
    same = down == across

    def column(row):
        return jnp.sum(jnp.where(same, row, jnp.zeros_like(row)), axis=1, keepdims=True)

    def row_of(col):
        return jnp.sum(jnp.where(same, col, jnp.zeros_like(col)), axis=0, keepdims=True)

    def slots(m):
        pos = jnp.sum(jnp.where(picks[m] == down, across, 0), axis=1, keepdims=True)
        pos_row = row_of(pos)
        block = lax.div(pos, quarter)
        before = (lax.div(pos_row, quarter) == block) & (pos_row < pos)
        found = []
        for e in range(n_e):
            named = jnp.zeros((1, toks), jnp.int32)
            for k in range(ids.shape[1]):
                named = named + jnp.where(ids[m, k:k + 1] == e, 1, 0)
            slot = jnp.sum(jnp.where(before, named, 0), axis=1, keepdims=True)
            kept = (column(named) > 0) & (slot < capacity)
            found.append(jnp.where(kept, block * capacity + slot, -1))
        return found

    def place(m):
        places = lax.broadcasted_iota(jnp.int32, (rows_ge, toks), 0)
        for e, target in enumerate(slots(m)):
            placing[m, e] = jnp.where(places == row_of(target), 1.0, 0.0).astype(BF16)

    def weigh(m):
        for e, target in enumerate(slots(m)):
            w_row = jnp.zeros((1, toks), F32)
            for k in range(ids.shape[1]):
                w_row = w_row + jnp.where(ids[m, k:k + 1] == e, weights[m, k:k + 1], 0.0)
            spread = lax.broadcasted_iota(jnp.int32, (toks, rows_ge), 1) == target
            w_col = jnp.where(spread, column(w_row), 0.0)
            high = w_col.astype(BF16)
            comb[m, e, :toks] = high
            comb[m, e, toks:] = (w_col - high.astype(F32)).astype(BF16)

    for load in small:
        load.wait()
    for load in loads:
        load.start()
    place(0)

    ends = jnp.where(p > 0, 1, 0) + jnp.where(p < n_p - 1, 1, 0)
    pl.semaphore_wait(barrier, n_e - 1 + n_a - 1 + pair - 1 + ends)

    def relay(m, k):
        return remote(fresh.at[m, k], h_in.at[m, k], out_sem.at[0], h_recv.at[m, k],
                      {"pipe": jnp.minimum(p + 1, n_p - 1)})

    def d_copy(m, d, k):
        return remote(send.at[m, d, k], x.at[m, r, z, k], out_sem.at[1], d_recv.at[m, d - 1, k],
                      {"expert": peer_e(d)})

    def f_copy(m, d, da, k):
        block = x.at[m, r, peer_e(d), k]
        return remote(block, block, out_sem.at[2], f_recv.at[m, d, da - 1, k],
                      {"tensor": rank_of(da, 0)})

    def c_copy(m, d, da, k):
        block = x.at[m, rank_of(da, 0), peer_e(d), k]
        return remote(block, block, out_sem.at[3], c_recv.at[m, half_of(d), da],
                      {"tensor": rank_of(0, 1)})

    def half_of(d):
        return [h for h, half in enumerate(halves) if d in half][0]

    def shared(m, h, da):
        block = x.at[m, 0, 0:len(halves[h])]
        return remote(block, block, out_sem.at[3], c_recv.at[m, h, da], {"tensor": rank_of(0, 1)})

    def p_copy(m, h, da):
        return remote(p_send.at[m, h, da], p_recv.at[m, h, da], out_sem.at[4],
                      p_sem.at[m, h, da], {"tensor": rank_of(0, 1)})

    def y_copy(m, d, da, k):
        return remote(y_send.at[m, da, d, k], y_recv.at[m, da, d, k], out_sem.at[5],
                      y_sem.at[m, d, da - 1, k], {"tensor": rank_of(da, 0)})

    def z_copy(m, d, k):
        return remote(z_send.at[m, k, d], ret.at[m, k, z], out_sem.at[6], z_sem.at[m, k],
                      {"expert": peer_e(d)})

    def returned(m, k):
        block = ret.at[m, k, 1:n_e]
        return remote(block, block, out_sem.at[6], z_sem.at[m, k], {"expert": peer_e(1)})

    def arrive(m, k, first):
        if first:
            first_load(m, k).wait()
        else:
            relay(m, k).wait_recv()

    def dispatch(m, blocks):
        for d, k in blocks:
            block = jnp.dot(placing[m, peer_e(d)], h_in[m, k], preferred_element_type=F32).astype(BF16)
            if d:
                send[m, d, k] = block
            else:
                x[m, r, z, k] = block
        for d, k in blocks:
            if d:
                d_copy(m, d, k).start()

    def forward(m, d, k):
        if d:
            d_copy(m, d, k).wait_recv()
        for da in range(1, n_a):
            f_copy(m, d, da, k).start()
        if pair > 1:
            c_copy(m, d, 0, k).start()

    def pass_on(m, d, k):
        for da in range(1, n_a):
            f_copy(m, d, da, k).wait_recv()
            if pair > 1:
                c_copy(m, d, da, k).start()

    squares = {}

    def gate(m, h, i):
        da, dc = ranks[i]
        if m == 0 and h == 0 and i == 0:
            loads[0].wait()
            loads[1].wait()
        if dc:
            shared(m, h, da).wait_recv()
        q = rank_of(da, dc)
        gq = uq = None
        ss = squares.get((m, h))
        for k in ks:
            xf = jnp.concatenate([x[m, q, peer_e(d), k].astype(F32) for d in halves[h]], axis=0)
            part = jnp.sum(xf * xf, axis=-1, keepdims=True)
            ss = part if ss is None else ss + part
            start = pl.multiple_of(q * width + k * sub, sub)
            xg = (xf * gains[0:1, pl.ds(start, sub)]).astype(BF16)
            g1 = jnp.dot(xg, wg[pl.ds(start, sub), :], preferred_element_type=F32)
            u1 = jnp.dot(xg, wu[pl.ds(start, sub), :], preferred_element_type=F32)
            gq = g1 if gq is None else gq + g1
            uq = u1 if uq is None else uq + u1
        squares[m, h] = ss
        if i == 0:
            g_acc[h] = gq
            u_acc[h] = uq
        else:
            g_acc[h] += gq
            u_acc[h] += uq

    def finish(m, h):
        if m == 0 and h == 0:
            loads[2].wait()
        inv = lax.rsqrt(squares[m, h] * (1.0 / (n_t * width)) + epsilon)
        g = g_acc[h] * inv
        hidden = (g / (1.0 + jnp.exp(-g)) * (u_acc[h] * inv)).astype(BF16)
        order = list(range(1, n_a)) + [0]
        for dc in list(range(1, pair)) + [0]:
            for da in order:
                for k in ks:
                    start = pl.multiple_of(rank_of(da, dc) * width + k * sub, sub)
                    part = jnp.dot(hidden, wd[:, pl.ds(start, sub)], preferred_element_type=F32)
                    if dc:
                        p_send[m, h, da, k] = part.astype(BF16)
                    else:
                        own[m, h, da, k] = part.astype(BF16)
            if dc:
                for da in order:
                    p_copy(m, h, da).start()

    def reduce_pair(m, h):
        for da in list(range(1, n_a)) + [0]:
            if pair > 1:
                p_copy(m, h, da).wait_recv()
            for i, d in enumerate(halves[h]):
                for k in ks:
                    part = slice(i * rows_ge, (i + 1) * rows_ge)
                    total = own[m, h, da, k, part].astype(F32)
                    if pair > 1:
                        total = total + p_recv[m, h, da, k, part].astype(F32)
                    y_send[m, da, d, k] = total.astype(BF16)
                    if da:
                        y_copy(m, d, da, k).start()

    def reduce_far(m, d, k):
        total = y_send[m, 0, d, k].astype(F32)
        for da in range(1, n_a):
            y_copy(m, d, da, k).wait_recv()
            total = total + y_recv[m, da, d, k].astype(F32)
        if d:
            z_send[m, k, d] = total.astype(BF16)
            z_copy(m, d, k).start()
        else:
            ret[m, k, z] = total.astype(BF16)

    def combine(m, k):
        returned(m, k).wait_recv()
        for d in range(n_e):
            e = peer_e(d)
            both = jnp.dot(comb[m, e], ret[m, k, e], preferred_element_type=F32)
            g_part = both[:toks] + both[toks:]
            update = g_part if d == 0 else update + g_part
        fresh[m, k] = (h_in[m, k].astype(F32) + update).astype(BF16)

        @pl.when(p < n_p - 1)
        def _():
            relay(m, k).start()

        out[0, m, :, k * sub:(k + 1) * sub] = fresh[m, k]

    def step(fn, *args):
        return functools.partial(fn, *args)

    near, rest = halves[0], [d for d in halves[1] if d]
    last = len(ranks)

    def gates(m, h, low, high):
        return [step(gate, m, h, i) for i in range(low, high)]

    def each(fn, m, blocks, parts_of=ks):
        return [step(fn, m, d, k) for d in blocks for k in parts_of]

    def spread(m, first):
        steps = []
        for k in ks:
            steps += [step(arrive, m, k, first), step(dispatch, m, [(d, k) for d in near])]
        for k in ks:
            steps += [step(dispatch, m, [(d, k) for d in rest])]
        return steps

    def keep(m):
        return [step(dispatch, m, [(0, k) for k in ks])] + each(forward, m, [0])

    early, late = list(ks)[:-1], list(ks)[-1:]

    def body(m, ahead, between, held):
        plan = each(forward, m, near) + gates(m, 0, 0, 1)
        plan += each(forward, m, rest, early) + each(pass_on, m, near[:1], early)
        plan += gates(m, 0, 1, pair) + ahead
        plan += each(pass_on, m, [0]) + each(pass_on, m, near[:1], late) + each(pass_on, m, near[1:])
        plan += gates(m, 0, pair, last - 1)
        plan += each(forward, m, rest, late) + held + between
        plan += gates(m, 1, 0, 1)
        plan += gates(m, 0, last - 1, last)
        plan += [step(finish, m, 0)]
        plan += each(pass_on, m, rest, early)
        plan += gates(m, 1, 1, pair)
        plan += [step(reduce_pair, m, 0)]
        plan += each(pass_on, m, rest, late)
        plan += gates(m, 1, pair, last)
        plan += [step(finish, m, 1)]
        return plan

    def joined(m):
        return [step(combine, m, k) for k in ks]

    def first_plan():
        close = near[1:]
        plan = spread(0, True) + keep(0)
        for m in range(1, micros):
            plan += [step(place, m)] + [step(arrive, m, k, True) for k in ks] + keep(m)
        for m in range(micros):
            more = range(m + 1, min(m + 2, micros))
            far = [step(dispatch, n, [(d, k) for d in near[:1] + rest for k in ks]) for n in more]
            side = [step(dispatch, n, [(d, k) for d in close for k in ks]) for n in more]
            if m == 0:
                moved = [go for n in more for go in each(forward, n, close)]
                plan += side + body(m, far, moved, [])
            else:
                plan += gates(m, 0, 0, 1) + joined(m - 1)
                plan += side + far + [go for n in more for go in each(forward, n, close)]
                plan += each(pass_on, m, [0] + close) + gates(m, 0, 1, pair) + each(pass_on, m, near[:1])
                plan += gates(m, 0, pair, last) + [step(finish, m, 0)]
                plan += each(pass_on, m, rest, early) + gates(m, 1, 0, pair) + [step(reduce_pair, m, 0)]
                plan += each(pass_on, m, rest, late) + gates(m, 1, pair, last) + [step(finish, m, 1)]
            plan += [step(weigh, m)]
            plan += each(reduce_far, m, near[:1], early) + [step(reduce_pair, m, 1)]
            plan += each(reduce_far, m, near[:1], late)
            for n in more:
                plan += each(forward, n, near[:1])
            plan += each(reduce_far, m, close)
            for n in more:
                plan += each(forward, n, rest)
            plan += each(reduce_far, m, rest + [0])
        return plan + joined(micros - 1)

    def later_plan():
        plan = [step(place, m) for m in range(1, micros)] + [step(weigh, m) for m in range(micros)]
        for m in range(micros):
            held = each(reduce_far, m - 1, near + rest + [0]) if m else []
            plan += spread(m, False) + keep(m) + body(m, [], [], held)
            if m + 1 == micros:
                plan += each(reduce_far, m, near[:1], early)
            plan += [step(reduce_pair, m, 1)]
            if m:
                plan += joined(m - 1)
        plan += each(reduce_far, micros - 1, near[:1], late)
        plan += each(reduce_far, micros - 1, near[1:] + rest + [0])
        return plan + joined(micros - 1)

    def follow(first):
        squares.clear()
        for go in first_plan() if first else later_plan():
            go()

    @pl.when(p == 0)
    def _():
        follow(True)

    @pl.when(p > 0)
    def _():
        follow(False)

    def sent(block, i):
        remote(block, block, out_sem.at[i], out_sem.at[i], {"expert": peer_e(1)}).wait_send()

    sent(send.at[:, 1:n_e], 1)
    if n_a > 1:
        sent(x.at[:, 0:n_a - 1], 2)
        sent(y_send.at[:, 1:n_a], 5)
    if pair > 1:
        sent(x.at[:, 0:n_a], 3)
        sent(p_send, 4)
    sent(z_send.at[:, :, 1:n_e], 6)
    @pl.when(p < n_p - 1)
    def _():
        sent(fresh, 0)


def local(mesh_shape, tokens, gains, route_ids, route_weights, picks, w_gate, w_up, w_down):
    n_p, n_t, n_e = mesh_shape
    micros, toks, model_width = tokens.shape
    route_count = route_ids.shape[3]
    quarter = toks // n_t
    capacity = 4 * quarter * route_count // (3 * n_e)
    width = model_width // n_t
    pair = 2 if n_t % 2 == 0 else 1
    parts = 2 if width % 256 == 0 else 1
    sub = width // parts
    n_a = n_t // pair
    rows_ge = -(-n_t * capacity // 8) * 8
    rows = (n_e + 1) // 2 * rows_ge
    hidden_width = w_gate.shape[3]

    ids = route_ids[0].transpose(0, 2, 1)
    weights = route_weights[0].transpose(0, 2, 1)
    order = picks[0]

    sizes = (micros, n_p, n_t, n_e, pair, parts, rows_ge, width, capacity)
    dma = pltpu.SemaphoreType.DMA
    pinned = pl.BlockSpec(memory_space=pl.ANY)
    return pl.pallas_call(
        functools.partial(layer_kernel, sizes),
        out_shape=pltpu.VMEM((1, micros, toks, width), BF16),
        in_specs=[pinned] * 8,
        out_specs=pl.BlockSpec(memory_space=pltpu.VMEM),
        scratch_shapes=[
            pltpu.VMEM(gains.shape, F32),
            pltpu.VMEM(ids.shape, jnp.int32),
            pltpu.VMEM(weights.shape, F32),
            pltpu.VMEM(order.shape, jnp.int32),
            pltpu.VMEM((micros, n_e, rows_ge, toks), BF16),
            pltpu.VMEM((micros, n_e, 2 * toks, rows_ge), BF16),
            pltpu.VMEM((micros, parts, toks, sub), BF16),
            pltpu.VMEM((micros, parts, toks, sub), BF16),
            pltpu.VMEM((micros, n_e, parts, rows_ge, sub), BF16),
            pltpu.VMEM((micros, n_t, n_e, parts, rows_ge, sub), BF16),
            pltpu.VMEM(w_gate.shape[2:], BF16),
            pltpu.VMEM(w_up.shape[2:], BF16),
            pltpu.VMEM(w_down.shape[2:], BF16),
            pltpu.VMEM((2, rows, hidden_width), F32),
            pltpu.VMEM((2, rows, hidden_width), F32),
            pltpu.VMEM((micros, 2, n_a, parts, rows, sub), BF16),
            pltpu.VMEM((micros, 2, n_a, parts, rows, sub), BF16),
            pltpu.VMEM((micros, 2, n_a, parts, rows, sub), BF16),
            pltpu.VMEM((micros, n_a, n_e, parts, rows_ge, sub), BF16),
            pltpu.VMEM((micros, n_a, n_e, parts, rows_ge, sub), BF16),
            pltpu.VMEM((micros, parts, n_e, rows_ge, sub), BF16),
            pltpu.VMEM((micros, parts, n_e, rows_ge, sub), BF16),
            dma((4,)), dma((3,)), dma((micros, parts)),
            dma((7,)), dma((micros, parts)), dma((micros, n_e - 1, parts)),
            dma((micros, n_e, n_a - 1, parts)), dma((micros, 2, n_a)), dma((micros, 2, n_a)),
            dma((micros, n_e, n_a - 1, parts)), dma((micros, parts)),
        ],
        compiler_params=pltpu.CompilerParams(
            collective_id=0, has_side_effects=True, vmem_limit_bytes=66584576
        ),
    )(tokens, gains, ids, weights, order, w_gate, w_up, w_down)


def solution(mesh):
    mesh_shape = (mesh.shape["pipe"], mesh.shape["tensor"], mesh.shape["expert"])
    return jax.shard_map(
        functools.partial(local, mesh_shape),
        mesh=mesh,
        in_specs=(
            P(None, "expert", None),
            P("pipe", None),
            P("pipe", None, "expert", None),
            P("pipe", None, "expert", None),
            P("pipe", None, "expert", None),
            P("pipe", "expert", None, "tensor"),
            P("pipe", "expert", None, "tensor"),
            P("pipe", "expert", "tensor", None),
        ),
        out_specs=P("pipe", None, "expert", "tensor"),
        check_vma=False,
    )
```
